32 devices in a mesh: row: 2 (over y), col: 8 (over z, x), layer: 2 (over core).
Axes of the slice: x: 2, y: 2, z: 4, core: 2. Of those that a mesh axis runs over, the one named last changes fastest.
Arguments:
- anomaly_x: bfloat16 [8, 4096, 4096], P(None, 'row', ('layer', 'col')), may hold values from -0.09375 to 0.09375
- anomaly_y: bfloat16 [8, 4096, 4096], P(None, 'col', ('layer', 'row')), may hold values from -6 to 6
Outputs:
- covariance: bfloat16 [8, 4096, 4096], P('layer', 'row', 'col')
The draws below stay inside these ranges and needn't reach their ends.
All inputs are finite; a program needn't handle non-finite values.
Results may differ from the reference program's by a relative error of at most 0.001.
Values may be sent and summed in bfloat16 or wider, within the bound.
A program may use at most 192 MiB of HBM per device.

```python
import jax
import jax.numpy as jnp
from jax import lax

BATCH = 8
NSTATE = 4096
MEMBERS = 4096


def raised(values, own_key, source, target, shards_of, factor):
    owner, partner = [(jnp.arange(values.shape[axis_at]) // (values.shape[axis_at] // shards_of)).reshape([-1 if axis == axis_at else 1 for axis in range(values.ndim)]) for axis_at in (source, target)]
    chosen = jax.random.permutation(own_key, shards_of)[partner]
    strong = (owner == chosen) | (owner == (partner + shards_of // 2) % shards_of)
    return jnp.where(strong, factor * values, values)


def steps_of(rng, dims, cuts, least, top_value):
    level, own = 1.0, jax.random.fold_in(rng, 6)
    for position, shards_of in cuts:
        steps = jnp.exp(jax.random.uniform(jax.random.fold_in(own, position), (shards_of,), jnp.float32, least / len(cuts), top_value / len(cuts)))
        level = level * jnp.repeat(steps, dims[position] // shards_of).reshape([-1 if axis == position else 1 for axis in range(len(dims))])
    return level


def noise(rng, shape, deviation, reach, pieces=(), held_as=jnp.bfloat16):
    gain = steps_of(rng, shape, pieces, -0.22, 0.18) if pieces else 1.0
    drawn = jax.random.normal(rng, shape, jnp.float32) * deviation * gain
    return jnp.minimum(jnp.maximum(drawn, -reach), reach).astype(held_as)


def heavy_noise(stream_key, dims, deviation, reach, shards, heavy, kind=jnp.bfloat16):
    result = deviation * jax.random.normal(stream_key, dims, jnp.float32)
    if shards:
        result = result * steps_of(stream_key, dims, shards, -0.22, 0.18)
    return jnp.clip(raised(result, jax.random.fold_in(stream_key, 3), *heavy), -reach, reach).astype(kind)


def setup_inputs(seed: int = 0) -> dict:
    key_of = jax.random.split(jax.random.key(seed), 3)
    return {
        "anomaly_x": noise(key_of[0], (BATCH, NSTATE, MEMBERS), MEMBERS ** -0.5, 0.09375, ((1, 2), (2, 16))),
        "anomaly_y": heavy_noise(key_of[1], (BATCH, NSTATE, MEMBERS), 1.0, 6.0, ((1, 8), (2, 4)), (2, 0, 4, 2.0)),
    }


def one_product(pair):
    left, right = pair
    return jnp.dot(left, right.T, preferred_element_type=jnp.float32).astype(jnp.bfloat16)


def reference(anomaly_x, anomaly_y):
    return lax.map(one_product, (anomaly_x, anomaly_y))
```

```python
import functools

import jax
import jax.numpy as jnp
from jax import lax
from jax.experimental import pallas as pl
from jax.experimental.pallas import tpu as pltpu
from jax.sharding import PartitionSpec as P

LANES = 128
MESH = pl.DeviceIdType.MESH
NT = (((1,), (1,)), ((), ()))


def gathered(anomaly_x, anomaly_y):
    panel_x = lax.all_gather(anomaly_x, "col", axis=2, tiled=True)
    partial_tile = jnp.einsum(
        "bik,bjk->bij",
        panel_x,
        lax.all_gather(anomaly_y, "row", axis=2, tiled=True),
        preferred_element_type=jnp.float32,
    )
    summed = lax.psum_scatter(partial_tile, "layer", scatter_dimension=0, tiled=True)
    return summed.astype(jnp.bfloat16)


def kernel(
    sizes, x_ref, y_ref, o_ref, xg, yg, og, rx, ry, ro, local_sem,
    x_send, x_recv, xf_send, xf_recv, y_send, y_recv, yf_send, yf_recv,
    r_send, r_recv, q_send, o_send, o_recv, op_send, op_recv, oq_send,
):
    rows, planes, lines, layers = sizes
    y, col, c = lax.axis_index("row"), lax.axis_index("col"), lax.axis_index("layer")
    z, x = col // lines, lax.rem(col, lines)
    depth_x, depth_y = x_ref.shape[2], y_ref.shape[2]
    height, width = x_ref.shape[1], y_ref.shape[1]
    group = depth_x * planes * lines
    relayed = planes == 4
    half = height // 2

    def plane(d):
        return lax.rem(z + d + planes, planes)

    def core(e):
        return lax.rem(c + e + layers, layers)

    def dev(yy, zz, xx, cc):
        return {"row": yy, "col": zz * lines + xx, "layer": cc}

    def xcols(cc, zz, xx):
        return pl.ds(pl.multiple_of(cc * group + (zz * lines + xx) * depth_x, depth_x), depth_x)

    def ycols(cc, yy):
        return pl.ds(pl.multiple_of(cc * group + yy * depth_y, depth_y), depth_y)

    def batch(zz, cc):
        return cc * planes + zz

    xline = [lax.rem(x + d, lines) for d in range(1, lines)]
    yline = [lax.rem(y + d, rows) for d in range(1, rows)]
    peers = [dev(y, plane(d), x, core(e)) for d in range(planes) for e in range(layers) if d or e]
    peers += [dev(y, z, xx, c) for xx in xline] + [dev(yy, z, x, c) for yy in yline]
    barrier = pltpu.get_barrier_semaphore()
    for peer in peers:
        pl.semaphore_signal(barrier, inc=1, device_id=peer, device_id_type=MESH)
    pl.semaphore_wait(barrier, len(peers))

    sent = []

    def push(src, dst, s, r, to):
        cp = pltpu.make_async_remote_copy(
            src_ref=src, dst_ref=dst, send_sem=s, recv_sem=r, device_id=to, device_id_type=MESH
        )
        cp.start()
        sent.append(cp)

    def landed(dst, s, r):
        pltpu.make_async_remote_copy(
            src_ref=dst, dst_ref=dst, send_sem=s, recv_sem=r, device_id=peers[0], device_id_type=MESH
        ).wait_recv()

    def send_x(d, e):
        push(x_ref.at[batch(plane(d), core(e))], xg.at[:, xcols(c, z, x)],
             x_send.at[d * layers + e], x_recv.at[d * layers + e], dev(y, plane(d), x, core(e)))

    def send_y(d, e):
        push(y_ref.at[batch(plane(d), core(e))], yg.at[d, :, ycols(c, y)],
             y_send.at[d * layers + e], y_recv.at[d * layers + e], dev(y, plane(d), x, core(e)))

    def forward_x(d, e, src=None):
        zone = xg.at[:, xcols(core(-e), plane(-d), x)]
        if src is None:
            landed(zone, x_send.at[d * layers + e], x_recv.at[d * layers + e])
        for j, xx in enumerate(xline):
            i = (d * layers + e) * len(xline) + j
            push(zone if src is None else src, zone, xf_send.at[i], xf_recv.at[i], dev(y, z, xx, c))

    def forward_y(d, e, src=None):
        zone = yg.at[d, :, ycols(core(-e), y)]
        if src is None:
            landed(zone, y_send.at[d * layers + e], y_recv.at[d * layers + e])
        for j, yy in enumerate(yline):
            i = (d * layers + e) * len(yline) + j
            push(zone if src is None else src, zone, yf_send.at[i], yf_recv.at[i], dev(yy, z, x, c))

    mine = batch(z, c)
    forward_x(0, 0, x_ref.at[mine])
    forward_y(0, 0, y_ref.at[mine])
    keep_x = pltpu.make_async_copy(x_ref.at[mine], xg.at[:, xcols(c, z, x)], local_sem.at[0])
    keep_y = pltpu.make_async_copy(y_ref.at[mine], yg.at[0, :, ycols(c, y)], local_sem.at[1])
    keep_x.start()
    keep_y.start()

    far = planes // 2
    near = [d for d in range(1, planes) if not (relayed and d == far)]
    if relayed:
        back = dev(y, plane(-1), x, c)
        push(x_ref.at[batch(plane(far), core(1))], rx, r_send.at[0], r_recv.at[0], back)
        push(y_ref.at[batch(plane(far), core(0))], ry, r_send.at[1], r_recv.at[1], back)
        send_x(far, 0)
        send_y(far, 1)
    for e in range(1, layers):
        send_x(0, e)
        send_y(0, e)
    for d in near:
        send_x(d, 0)
        send_y(d, 0)
    if relayed:
        i = far * layers
        landed(rx, r_send.at[0], r_recv.at[0])
        push(rx, xg.at[:, xcols(c, plane(1), x)], q_send.at[0], x_recv.at[i + 1],
             dev(y, plane(-1), x, core(1)))
        landed(ry, r_send.at[1], r_recv.at[1])
        push(ry, yg.at[far, :, ycols(c, y)], q_send.at[1], y_recv.at[i],
             dev(y, plane(-1), x, c))
    for e in range(1, layers):
        for d in near:
            send_x(d, e)
            send_y(d, e)

    for e in range(1, layers):
        forward_x(0, e)
        forward_y(0, e)
    order = [(d, 0) for d in near]
    if relayed:
        order = [(far, 0, "x"), (far, 1, "y")] + order + [(far, 1, "x"), (far, 0, "y")]
    order += [(d, e) for e in range(1, layers) for d in near]
    for step in order:
        which = step[2] if len(step) > 2 else "xy"
        if "x" in which:
            forward_x(step[0], step[1])
        if "y" in which:
            forward_y(step[0], step[1])

    keep_x.wait()
    keep_y.wait()
    for d in range(planes):
        for e in range(layers):
            for j in range(len(xline)):
                xx = lax.rem(x - (j + 1) + lines, lines)
                i = (d * layers + e) * len(xline) + j
                landed(xg.at[:, xcols(core(-e), plane(-d), xx)], xf_send.at[i], xf_recv.at[i])
    for d in range(planes):
        for e in range(layers):
            for j in range(len(yline)):
                yy = lax.rem(y - (j + 1) + rows, rows)
                i = (d * layers + e) * len(yline) + j
                landed(yg.at[d, :, ycols(core(-e), yy)], yf_send.at[i], yf_recv.at[i])

    tile = min(height, 256)

    def multiply(d, low, high):
        def body(r, _):
            at = pl.ds(pl.multiple_of(r * tile, tile), tile)
            og[d, at, :] = lax.dot_general(
                xg[at, :], yg[d], NT, preferred_element_type=jnp.float32
            ).astype(jnp.bfloat16)
            return 0

        lax.fori_loop(low // tile, high // tile, body, 0)

    top, low_half = pl.ds(0, half), pl.ds(half, half)
    if relayed:
        multiply(far, half, height)
        push(og.at[far, low_half], ro, op_send.at[0], op_recv.at[0], dev(y, plane(-1), x, c))
        multiply(far, 0, half)
        push(og.at[far, top], o_ref.at[z, top], o_send.at[far], o_recv.at[far], dev(y, plane(-far), x, c))
    for d in near:
        multiply(d, 0, height)
        push(og.at[d], o_ref.at[z], o_send.at[d], o_recv.at[d], dev(y, plane(-d), x, c))
    if relayed:
        landed(ro, op_send.at[0], op_recv.at[0])
        push(ro, o_ref.at[plane(1), low_half], oq_send.at[0], op_recv.at[1], dev(y, plane(-1), x, c))
    multiply(0, 0, height)
    keep = pltpu.make_async_copy(og.at[0], o_ref.at[z], local_sem.at[2])
    keep.start()
    for d in near:
        landed(o_ref.at[plane(d)], o_send.at[d], o_recv.at[d])
    if relayed:
        landed(o_ref.at[plane(far), top], o_send.at[far], o_recv.at[far])
        landed(o_ref.at[plane(far), low_half], oq_send.at[0], op_recv.at[1])
    keep.wait()
    for cp in sent:
        cp.wait_send()


def routed(sizes, anomaly_x, anomaly_y):
    rows, planes, lines, layers = sizes
    batches, height, depth_x = anomaly_x.shape
    width, depth_y = anomaly_y.shape[1:]
    members = depth_y * rows * layers
    blocks = planes * layers
    dma = pltpu.SemaphoreType.DMA
    any_ = pl.BlockSpec(memory_space=pl.ANY)
    fx, fy = max(1, blocks * (lines - 1)), max(1, blocks * (rows - 1))
    kind = anomaly_x.dtype
    return pl.pallas_call(
        functools.partial(kernel, sizes),
        out_shape=jax.ShapeDtypeStruct((planes, height, width), jnp.bfloat16),
        in_specs=[any_, any_],
        out_specs=any_,
        scratch_shapes=[
            pltpu.VMEM((height, members), kind),
            pltpu.VMEM((planes, width, members), kind),
            pltpu.VMEM((planes, height, width), jnp.bfloat16),
            pltpu.VMEM((height, depth_x), kind),
            pltpu.VMEM((width, depth_y), kind),
            pltpu.VMEM((height // 2, width), jnp.bfloat16),
            dma((3,)),
            dma((blocks,)), dma((blocks,)), dma((fx,)), dma((fx,)),
            dma((blocks,)), dma((blocks,)), dma((fy,)), dma((fy,)),
            dma((2,)), dma((2,)), dma((2,)),
            dma((planes,)), dma((planes,)), dma((1,)), dma((2,)), dma((1,)),
        ],
        compiler_params=pltpu.CompilerParams(
            collective_id=0, has_side_effects=True, vmem_limit_bytes=60 * 2**20
        ),
    )(anomaly_x, anomaly_y)


def on_device(mesh, anomaly_x, anomaly_y):
    rows, cols, layers = (mesh.shape[name] for name in ("row", "col", "layer"))
    batches, _, depth_x = anomaly_x.shape
    planes = batches // layers
    if layers != 2 or batches % layers or cols % planes or depth_x % LANES:
        return gathered(anomaly_x, anomaly_y)
    return routed((rows, planes, cols // planes, layers), anomaly_x, anomaly_y)


def solution(mesh):
    placed = (P(None, "row", ("layer", "col")), P(None, "col", ("layer", "row")))
    return jax.shard_map(
        functools.partial(on_device, mesh),
        mesh=mesh, in_specs=placed, out_specs=P("layer", "row", "col"), check_vma=False,
    )
```

```python
import functools

import jax
import jax.numpy as jnp
from jax import lax
from jax.experimental import pallas as pl
from jax.experimental.pallas import tpu as pltpu
from jax.sharding import PartitionSpec as P

LANES = 128
HALVES = 2
MESH = pl.DeviceIdType.MESH
NT = (((1,), (1,)), ((), ()))


def gathered(anomaly_x, anomaly_y):
    panel_x = lax.all_gather(anomaly_x, "col", axis=2, tiled=True)
    partial_tile = jnp.einsum(
        "bik,bjk->bij",
        panel_x,
        lax.all_gather(anomaly_y, "row", axis=2, tiled=True),
        preferred_element_type=jnp.float32,
    )
    summed = lax.psum_scatter(partial_tile, "layer", scatter_dimension=0, tiled=True)
    return summed.astype(jnp.bfloat16)


def kernel(
    sizes, x_ref, y_ref, o_ref, xg, yg, og, local_sem,
    x_send, x_recv, xf_send, xf_recv, y_send, y_recv, yf_send, yf_recv, o_send, o_recv,
):
    rows, planes, lines, layers = sizes
    y, col, c = lax.axis_index("row"), lax.axis_index("col"), lax.axis_index("layer")
    z, x = col // lines, lax.rem(col, lines)
    depth_x, depth_y = x_ref.shape[2], y_ref.shape[2]
    height = x_ref.shape[1]
    group = depth_x * planes * lines
    steps = HALVES
    span = planes // HALVES
    q = lax.rem(z, span)
    base = z - q

    def plane(d):
        return lax.rem(z + d + planes, planes)

    def near(d):
        return lax.rem(q + d + span, span)

    def core(e):
        return lax.rem(c + e + layers, layers)

    def dev(yy, zz, xx, cc):
        return {"row": yy, "col": zz * lines + xx, "layer": cc}

    def xcols(cc, zz, xx):
        return pl.ds(pl.multiple_of(cc * group + (zz * lines + xx) * depth_x, depth_x), depth_x)

    def ycols(cc, yy):
        return pl.ds(pl.multiple_of(cc * group + yy * depth_y, depth_y), depth_y)

    def batch(qq, cc, s):
        return cc * planes + qq * steps + s

    xline = [lax.rem(x + d, lines) for d in range(1, lines)]
    yline = [lax.rem(y + d, rows) for d in range(1, rows)]
    peers = [dev(y, plane(d), x, core(e)) for d in range(planes) for e in range(layers) if d or e]
    peers += [dev(y, z, xx, c) for xx in xline] + [dev(yy, z, x, c) for yy in yline]
    barrier = pltpu.get_barrier_semaphore()
    for peer in peers:
        pl.semaphore_signal(barrier, inc=1, device_id=peer, device_id_type=MESH)
    pl.semaphore_wait(barrier, len(peers))

    sent = []

    def push(src, dst, s, r, to):
        cp = pltpu.make_async_remote_copy(
            src_ref=src, dst_ref=dst, send_sem=s, recv_sem=r, device_id=to, device_id_type=MESH
        )
        cp.start()
        sent.append(cp)

    def landed(dst, s, r):
        pltpu.make_async_remote_copy(
            src_ref=dst, dst_ref=dst, send_sem=s, recv_sem=r, device_id=peers[0], device_id_type=MESH
        ).wait_recv()

    def send_x(s, d, e):
        i = (s * planes + d) * layers + e
        to = plane(d)
        push(x_ref.at[batch(lax.rem(to, span), core(e), s)], xg.at[s, :, xcols(c, z, x)],
             x_send.at[i], x_recv.at[i], dev(y, to, x, core(e)))

    def send_y(s, d, e):
        i = (s * span + d) * layers + e
        push(y_ref.at[batch(near(d), core(e), s)], yg.at[s, d, :, ycols(c, y)],
             y_send.at[i], y_recv.at[i], dev(y, base + near(d), x, core(e)))

    def forward_x(s, d, e, src=None):
        i = (s * planes + d) * layers + e
        zone = xg.at[s, :, xcols(core(-e), plane(-d), x)]
        if src is None:
            landed(zone, x_send.at[i], x_recv.at[i])
        for j, xx in enumerate(xline):
            k = i * len(xline) + j
            push(zone if src is None else src, zone, xf_send.at[k], xf_recv.at[k], dev(y, z, xx, c))

    def forward_y(s, d, e, src=None):
        i = (s * span + d) * layers + e
        zone = yg.at[s, d, :, ycols(core(-e), y)]
        if src is None:
            landed(zone, y_send.at[i], y_recv.at[i])
        for j, yy in enumerate(yline):
            k = i * len(yline) + j
            push(zone if src is None else src, zone, yf_send.at[k], yf_recv.at[k], dev(yy, z, x, c))

    far = planes // 2
    order = [(far, e) for e in range(layers)]
    order += [(d, e) for d in range(1, planes) if d != far for e in range(layers)]
    keeps = []
    for s in range(steps):
        own = batch(q, c, s)
        forward_x(s, 0, 0, x_ref.at[own])
        forward_y(s, 0, 0, y_ref.at[own])
        keep_x = pltpu.make_async_copy(x_ref.at[own], xg.at[s, :, xcols(c, z, x)], local_sem.at[2 * s])
        keep_y = pltpu.make_async_copy(y_ref.at[own], yg.at[s, 0, :, ycols(c, y)], local_sem.at[2 * s + 1])
        keep_x.start()
        keep_y.start()
        keeps.append((keep_x, keep_y))
        for e in range(1, layers):
            send_x(s, 0, e)
            send_y(s, 0, e)
        for d, e in order:
            send_x(s, d, e)
            if d < span:
                send_y(s, d, e)

    tile = min(height, 256)

    def multiply(s, d):
        def body(r, _):
            at = pl.ds(pl.multiple_of(r * tile, tile), tile)
            og[s, d, at, :] = lax.dot_general(
                xg[s, at, :], yg[s, d], NT, preferred_element_type=jnp.float32
            ).astype(jnp.bfloat16)
            return 0

        lax.fori_loop(0, height // tile, body, 0)

    outs = []
    for s in range(steps):
        for e in range(1, layers):
            forward_x(s, 0, e)
            forward_y(s, 0, e)
        for d in list(range(1, far)) + list(range(far + 1, planes)) + [far]:
            for e in range(layers):
                forward_x(s, d, e)
                if d < span:
                    forward_y(s, d, e)
        for keep in keeps[s]:
            keep.wait()
        for d in range(planes):
            for e in range(layers):
                for j in range(len(xline)):
                    xx = lax.rem(x - (j + 1) + lines, lines)
                    k = ((s * planes + d) * layers + e) * len(xline) + j
                    landed(xg.at[s, :, xcols(core(-e), plane(-d), xx)], xf_send.at[k], xf_recv.at[k])
        for d in range(span):
            for e in range(layers):
                for j in range(len(yline)):
                    yy = lax.rem(y - (j + 1) + rows, rows)
                    k = ((s * span + d) * layers + e) * len(yline) + j
                    landed(yg.at[s, d, :, ycols(core(-e), yy)], yf_send.at[k], yf_recv.at[k])
        for d in list(range(1, span)):
            multiply(s, d)
            push(og.at[s, d], o_ref.at[q * steps + s], o_send.at[s * span + d], o_recv.at[s * span + d],
                 dev(y, base + near(-d), x, c))
        multiply(s, 0)
        keep = pltpu.make_async_copy(og.at[s, 0], o_ref.at[q * steps + s], local_sem.at[2 * steps + s])
        keep.start()
        outs.append(keep)
    for s in range(steps):
        for d in range(1, span):
            landed(o_ref.at[near(d) * steps + s], o_send.at[s * span + d], o_recv.at[s * span + d])
        outs[s].wait()
    for cp in sent:
        cp.wait_send()


def routed(sizes, anomaly_x, anomaly_y):
    rows, planes, lines, layers = sizes
    _, height, depth_x = anomaly_x.shape
    width, depth_y = anomaly_y.shape[1:]
    members = depth_y * rows * layers
    span, steps = planes // HALVES, HALVES
    bx, by = steps * planes * layers, steps * span * layers
    dma = pltpu.SemaphoreType.DMA
    any_ = pl.BlockSpec(memory_space=pl.ANY)
    fx, fy = max(1, bx * (lines - 1)), max(1, by * (rows - 1))
    kind = anomaly_x.dtype
    return pl.pallas_call(
        functools.partial(kernel, sizes),
        out_shape=jax.ShapeDtypeStruct((planes, height, width), jnp.bfloat16),
        in_specs=[any_, any_],
        out_specs=any_,
        scratch_shapes=[
            pltpu.VMEM((steps, height, members), kind),
            pltpu.VMEM((steps, span, width, members), kind),
            pltpu.VMEM((steps, span, height, width), jnp.bfloat16),
            dma((3 * steps,)),
            dma((bx,)), dma((bx,)), dma((fx,)), dma((fx,)),
            dma((by,)), dma((by,)), dma((fy,)), dma((fy,)),
            dma((steps * span,)), dma((steps * span,)),
        ],
        compiler_params=pltpu.CompilerParams(
            collective_id=0, has_side_effects=True, vmem_limit_bytes=63 * 2**20
        ),
    )(anomaly_x, anomaly_y)


def on_device(mesh, anomaly_x, anomaly_y):
    rows, cols, layers = (mesh.shape[name] for name in ("row", "col", "layer"))
    batches, _, depth_x = anomaly_x.shape
    planes = batches // layers
    if batches % layers or planes % HALVES or cols % planes or depth_x % LANES:
        return gathered(anomaly_x, anomaly_y)
    return routed((rows, planes, cols // planes, layers), anomaly_x, anomaly_y)


def solution(mesh):
    placed = (P(None, "row", ("layer", "col")), P(None, "col", ("layer", "row")))
    return jax.shard_map(
        functools.partial(on_device, mesh),
        mesh=mesh, in_specs=placed, out_specs=P("layer", "row", "col"), check_vma=False,
    )
```
